32 devices in a mesh: row: 8 (over z, y), col: 4 (over x, core).
Axes of the slice: x: 2, y: 2, z: 4, core: 2. Of those that a mesh axis runs over, the one named last changes fastest.
Arguments:
- amplitudes: float32 [128, 512, 512], P(('row', 'col')), may hold values from -6 to 6
- integrals: float32 [512, 1024, 1024], P(('row', 'col')), may hold values from -0.01171875 to 0.01171875
- coupling: float32 [512, 32, 1024], P(('row', 'col')), may hold values from -0.046875 to 0.046875
- task_table: int32 [32, 16, 2], replicated, may hold values from -1 to 15, as said below
Outputs:
- residual: float32 [128, 1024], P(('row', 'col'))
The draws below stay inside these ranges and needn't reach their ends.
Inputs may be any that keep to these rules, and one draw needn't show every extreme that they name: `task_table`: every virtual tile pair (C, D), C and D in 0 to 15, appears in exactly one slot. In each device's row the valid slots come first and the rest hold -1 in both entries. Some device has all 16 slots valid and some device has none. `integrals`: slots that task_table marks -1 are not read.
All inputs are finite; a program needn't handle non-finite values.
Results may differ from the reference program's by a relative error of at most 0.0003.
Values sent between devices are 32-bit elements; how exact they have to be, the bound alone decides.
A program may use at most 192 MiB of HBM per device.

```python
import jax
import jax.numpy as jnp
from jax import lax

O = 32
V = 512
TB = 32
OW = 4
NVT = 16
TILES = 256
SLOTS = 16
SLOTS_ALL = 512
ROWS = 128
DEVICES = 32


def draw_task_table(key, part):
    first, second, third = jax.random.split(jax.random.fold_in(key, 11), 3)
    halves = DEVICES // 2
    split_sizes = jax.random.randint(first, (halves,), 0, SLOTS + 1).astype(jnp.int32)
    split_sizes = split_sizes.at[0].set(SLOTS)
    paired = jnp.stack([split_sizes, SLOTS - split_sizes], axis=1).reshape(DEVICES)
    device_order = jax.random.permutation(second, DEVICES)
    tallies = jnp.zeros((DEVICES,), jnp.int32).at[device_order].set(paired)
    offsets = jnp.cumsum(tallies) - tallies
    shuffled = jax.random.permutation(third, TILES).astype(jnp.int32)
    slot_range = jnp.arange(SLOTS, dtype=jnp.int32)
    positions = jnp.clip(offsets[:, None] + slot_range[None, :], 0, TILES - 1)
    valid = slot_range[None, :] < tallies[:, None]
    chosen = shuffled[positions]
    upper = jnp.where(valid, chosen // NVT, -1)
    lower = jnp.where(valid, chosen % NVT, -1)
    return jnp.stack([upper, lower], axis=-1).astype(jnp.int32)


def levels(rng, extent, cuts, smallest, largest):
    factor_of, own = 1.0, jax.random.fold_in(rng, 6)
    for position, shards_of in cuts:
        draws = jnp.exp(jax.random.uniform(jax.random.fold_in(own, position), (shards_of,), jnp.float32, smallest / len(cuts), largest / len(cuts)))
        factor_of = factor_of * jnp.repeat(draws, extent[position] // shards_of).reshape([-1 if axis == position else 1 for axis in range(len(extent))])
    return factor_of


def centred(own_key, shape, scale, reach, cuts=(), kind=jnp.bfloat16):
    factor_of = levels(own_key, shape, cuts, -0.22, 0.18) if cuts else 1.0
    values = jax.random.normal(own_key, shape, jnp.float32) * scale * factor_of
    return jnp.minimum(jnp.maximum(values, -reach), reach).astype(kind)


def setup_inputs(seed: int = 0) -> dict:
    arg_keys = jax.random.split(jax.random.key(seed), 5)
    amplitudes = centred(arg_keys[0], (ROWS, V, V), 1.0, 6.0, ((0, 32),), jnp.float32)
    integrals = centred(arg_keys[1], (SLOTS_ALL, TB * TB, TB * TB), (V * V) ** -0.5, 0.01171875, ((0, 32),), jnp.float32)
    coupling = centred(arg_keys[2], (V, O, O * TB), (V * O) ** -0.5, 0.046875, ((0, 32),), jnp.float32)
    task_table = draw_task_table(jax.random.fold_in(arg_keys[4], 71), 0)
    return dict(amplitudes=amplitudes, integrals=integrals, coupling=coupling, task_table=task_table)


def reference(amplitudes, integrals, coupling, task_table):
    flat = task_table.reshape(SLOTS_ALL, 2)
    valid = flat[:, 0] >= 0
    pair_ids = jnp.where(valid, flat[:, 0] * NVT + flat[:, 1], TILES).astype(jnp.int32)
    inverse = jnp.zeros((TILES + 1,), jnp.int32).at[pair_ids].set(jnp.arange(SLOTS_ALL, dtype=jnp.int32))[:TILES]

    def add_pair(partial_value, tile_index):
        upper = ((tile_index // NVT) * TB).astype(jnp.int32)
        lower = ((tile_index % NVT) * TB).astype(jnp.int32)
        columns = lax.dynamic_slice(amplitudes, (jnp.int32(0), upper, lower), (ROWS, TB, TB)).reshape(ROWS, TB * TB)
        integral_tile = integrals[inverse[tile_index]]
        product = lax.dot_general(columns, integral_tile, (((1,), (1,)), ((), ())), precision=lax.Precision.HIGHEST, preferred_element_type=jnp.float32)
        return partial_value + product, None

    ladder, _ = lax.scan(add_pair, jnp.zeros((ROWS, TB * TB), jnp.float32), jnp.arange(TILES, dtype=jnp.int32))
    regrouped = jnp.transpose(amplitudes[:, :TB, :].reshape(OW, O, TB, V), (0, 2, 3, 1)).reshape(OW * TB, V * O)
    hole_term = jnp.dot(regrouped, coupling.reshape(V * O, O * TB), precision=lax.Precision.HIGHEST, preferred_element_type=jnp.float32)
    hole_term = jnp.transpose(hole_term.reshape(OW, TB, O, TB), (0, 2, 1, 3)).reshape(ROWS, TB * TB)
    return ladder + hole_term
```

```python
import functools

import jax
import jax.numpy as jnp
from jax import lax
from jax.experimental import pallas as pl
from jax.experimental.pallas import tpu as pltpu
from jax.sharding import PartitionSpec as P

TB = 32
NVT = 16
LANES = 128
GROUP = LANES // TB
SUB = TB * TB // LANES


def pack_kernel(local_rows, slots_all, ids_ref, amp_ref, out_ref, held, sems):
    wide = NVT * TB
    copies = []
    for h in range(wide // LANES):
        for r in range(local_rows):
            n = h * local_rows + r
            copies.append(
                pltpu.make_async_copy(
                    amp_ref.at[r, :, pl.ds(h * LANES, LANES)],
                    held.at[pl.ds(n * wide, wide), :],
                    sems.at[n],
                )
            )
    for copy in copies:
        copy.start()
    for copy in copies:
        copy.wait()
    chunk = lax.broadcasted_iota(jnp.int32, (SUB, LANES), 1) // TB

    def one_slot(k, carry):
        pair = ids_ref[k]

        @pl.when(pair >= 0)
        def _():
            upper = pair // NVT
            lower = pair % NVT
            h = lower // GROUP
            low = lower % GROUP
            for r in range(local_rows):
                base = (h * local_rows + r) * wide + upper * TB
                value = jnp.zeros((SUB, LANES), jnp.float32)
                for j in range(GROUP):
                    x = held[pl.ds(base + j, SUB, stride=GROUP), :]
                    x = pltpu.roll(x, ((j - low + GROUP) % GROUP) * TB, 1)
                    value = jnp.where(chunk == j, x, value)
                out_ref[k, pl.ds(r * SUB, SUB), :] = value

        return carry

    lax.fori_loop(0, slots_all, one_slot, 0)


def pack(amplitudes, ids, slots_all):
    local_rows = amplitudes.shape[0]
    groups = NVT * TB // LANES
    return pl.pallas_call(
        functools.partial(pack_kernel, local_rows, slots_all),
        out_shape=jax.ShapeDtypeStruct((slots_all, local_rows * SUB, LANES), jnp.float32),
        in_specs=[
            pl.BlockSpec(memory_space=pltpu.SMEM),
            pl.BlockSpec(memory_space=pl.ANY),
        ],
        out_specs=pl.BlockSpec(memory_space=pltpu.VMEM),
        scratch_shapes=[
            pltpu.VMEM((groups * local_rows * NVT * TB, LANES), jnp.float32),
            pltpu.SemaphoreType.DMA((groups * local_rows,)),
        ],
        compiler_params=pltpu.CompilerParams(vmem_limit_bytes=32 * 1024 * 1024),
        name="pack",
    )(ids, amplitudes)


def ladder_kernel(rows, count_ref, a_ref, v_ref, out_ref, flat, both, total):
    s = pl.program_id(0)

    @pl.when(s == 0)
    def _():
        total[...] = jnp.zeros_like(total)

    @pl.when(s < count_ref[0])
    def _():
        flat[...] = a_ref[:, 0].reshape(rows * SUB, LANES)
        for k in range(SUB):
            a = flat[pl.ds(k, rows, stride=SUB), :]
            high = a.astype(jnp.bfloat16)
            low = (a - high.astype(jnp.float32)).astype(jnp.bfloat16)
            both[pl.ds(0, rows), pl.ds(k * LANES, LANES)] = high
            both[pl.ds(rows, rows), pl.ds(k * LANES, LANES)] = low
        dims = (((1,), (1,)), ((), ()))
        step = 256
        for i in range(TB * TB // step):
            part = pl.ds(i * step, step)
            v = v_ref[0, part, :]
            vh = v.astype(jnp.bfloat16)
            vl = (v - vh.astype(jnp.float32)).astype(jnp.bfloat16)
            b = both[...]
            total[part, :] += lax.dot_general(
                vh, b, dims, preferred_element_type=jnp.float32
            ) + lax.dot_general(vl, b, dims, preferred_element_type=jnp.float32)

    @pl.when(s == pl.num_programs(0) - 1)
    def _():
        out_ref[...] = (total[:, :rows] + total[:, rows:]).T


def ladder_of(arrived, integrals, count):
    devices_all, slot_total, depth, _ = arrived.shape
    rows = devices_all * depth // SUB
    size = TB * TB

    def at(s, count_ref):
        return jnp.minimum(s, jnp.maximum(count_ref[0] - 1, 0))

    return pl.pallas_call(
        functools.partial(ladder_kernel, rows),
        out_shape=jax.ShapeDtypeStruct((rows, size), jnp.float32),
        grid_spec=pltpu.PrefetchScalarGridSpec(
            num_scalar_prefetch=1,
            grid=(slot_total,),
            in_specs=[
                pl.BlockSpec((devices_all, 1, depth, LANES), lambda s, c: (0, at(s, c), 0, 0)),
                pl.BlockSpec((1, size, size), lambda s, c: (at(s, c), 0, 0)),
            ],
            out_specs=pl.BlockSpec((rows, size), lambda s, c: (0, 0)),
            scratch_shapes=[
                pltpu.VMEM((rows * SUB, LANES), jnp.float32),
                pltpu.VMEM((2 * rows, size), jnp.bfloat16),
                pltpu.VMEM((size, 2 * rows), jnp.float32),
            ],
        ),
        compiler_params=pltpu.CompilerParams(
            dimension_semantics=("arbitrary",), vmem_limit_bytes=32 * 1024 * 1024
        ),
        name="ladder",
    )(count, arrived, integrals)


def body(amplitudes, integrals, coupling, task_table):
    devices_all = lax.axis_size("row") * lax.axis_size("col")
    local_rows = amplitudes.shape[0]
    slot_total = integrals.shape[0]
    total_rows = devices_all * local_rows
    upper, lower = task_table[:, :, 0], task_table[:, :, 1]
    ids = jnp.where(upper >= 0, upper * NVT + lower, -1)

    first_tile = amplitudes[:, :TB, :]
    pieces = lax.all_to_all(first_tile, ("row", "col"), split_axis=2, concat_axis=0, tiled=True)
    outgoing = pack(amplitudes, ids.reshape(-1), devices_all * slot_total).reshape(
        devices_all, slot_total * local_rows * SUB, LANES
    )
    arrived = lax.all_to_all(outgoing, ("row", "col"), split_axis=0, concat_axis=0, tiled=True)
    arrived = arrived.reshape(devices_all, slot_total, local_rows * SUB, LANES)

    own_index = lax.axis_index(("row", "col"))
    own_ids = lax.dynamic_index_in_dim(ids, own_index, 0, keepdims=False)
    count = jnp.sum((own_ids >= 0).astype(jnp.int32)).reshape(1)
    ladder = ladder_of(arrived, integrals, count)

    width_part = pieces.shape[2]
    occupied = coupling.shape[1]
    window = total_rows // occupied
    regrouped = jnp.transpose(
        pieces.reshape(window, occupied, TB, width_part), (0, 2, 3, 1)
    ).reshape(window * TB, width_part * occupied)
    coupling_rows = coupling.reshape(width_part * occupied, occupied * TB)
    hole_term = jnp.dot(
        regrouped,
        coupling_rows,
        precision=lax.Precision.HIGHEST,
        preferred_element_type=jnp.float32,
    )
    hole_term = jnp.transpose(hole_term.reshape(window, TB, occupied, TB), (0, 2, 1, 3)).reshape(
        total_rows, TB * TB
    )
    partial = (ladder + hole_term).reshape(devices_all, local_rows * SUB, LANES)
    shares = lax.all_to_all(partial, ("row", "col"), split_axis=0, concat_axis=0, tiled=True)
    return jnp.sum(shares, axis=0).reshape(local_rows, TB * TB)


def solution(mesh):
    in_specs = (
        P(("row", "col"), None, None),
        P(("row", "col"), None, None),
        P(("row", "col"), None, None),
        P(),
    )
    out_specs = P(("row", "col"), None)
    return jax.shard_map(body, mesh=mesh, in_specs=in_specs, out_specs=out_specs, check_vma=False)
```
